128 devices in a mesh: seq: 16 (over y, z_lo, core), zero: 8 (over x, z_hi).
Axes of the slice: x: 4, y: 4, z: 4 (z_hi: 2, z_lo: 2; z = z_hi * 2 + z_lo), core: 2. Of those that a mesh axis runs over, the one named last changes fastest.
Arguments:
- hidden: bfloat16 [8, 2048, 1280], P('zero', 'seq'), may hold values from -6 to 6
- output_grad: bfloat16 [8, 2048, 2560], P('zero', 'seq'), may hold values from -6 to 6
- input_weight: bfloat16 [1280, 2856], P('zero'), may hold values from -0.15625 to 0.15625
- step_bias: float32 [40], replicated, may hold values from -7 to -2
- decay_log: float32 [40], replicated, may hold values from -4 to 1
- skip_gain: float32 [40], replicated, may hold values from 0.5 to 1.5
Outputs:
- hidden_grad: bfloat16 [8, 2048, 1280], P('zero', 'seq')
- weight_grad: float32 [1280, 2856], P(('seq', 'zero'))
- head_grads: float32 [3, 40], replicated
The draws below stay inside these ranges and needn't reach their ends.
All inputs are finite; a program needn't handle non-finite values.
Results may differ from the reference program's by a relative error of at most 0.0049.
Values may be sent and summed in bfloat16 or wider, within the bound.
No kernel may reach another device: no remote copies, remote signals or barrier semaphores. Data moves between devices by JAX's collectives and lax.ppermute only.
A program may use at most 192 MiB of HBM per device.

```python
import jax
import jax.numpy as jnp
from jax import lax

D = 1280
HEADS = 40
HEAD_DIM = 64
STATE = 128
GROUP = 128
INNER = 2560
PROJ = 2856
LENGTH = 2048
SEQS = 8


def levels(key, shape, split, smallest, top_value):
    loudness = 1.0
    for position, blocks in split:
        steps = jax.random.uniform(jax.random.fold_in(jax.random.fold_in(key, 6), position), (blocks,), jnp.float32, smallest / len(split), top_value / len(split))
        loudness = loudness * jnp.repeat(jnp.exp(steps), shape[position] // blocks).reshape((-1,) + (1,) * (len(shape) - 1 - position))
    return loudness


def normal_values(stream_key, shape, deviation, bound, split=(), dtype=jnp.bfloat16):
    drawn = jax.random.normal(stream_key, shape, jnp.float32) * deviation
    if len(split) > 0:
        drawn = levels(stream_key, shape, split, -0.22, 0.18) * drawn
    return jnp.clip(drawn, min=-bound, max=bound).astype(dtype)


def setup_inputs(seed: int = 0) -> dict:
    seeds = jax.random.split(jax.random.key(seed), 7)
    return {
        "hidden": normal_values(seeds[0], (SEQS, LENGTH, D), 1.0, 6.0, ((0, 8), (1, 16))),
        "output_grad": normal_values(seeds[1], (SEQS, LENGTH, INNER), 1.0, 6.0, ((0, 8), (1, 16))),
        "input_weight": normal_values(seeds[2], (D, PROJ), D ** -0.5, 0.15625, ((0, 8),)),
        "step_bias": jnp.clip(jax.random.uniform(seeds[3], (HEADS,), jnp.float32, -7.0, -2.0), -7.0, -2.0),
        "decay_log": jnp.clip(jax.random.uniform(seeds[4], (HEADS,), jnp.float32, -4.0, 1.0), -4.0, 1.0),
        "skip_gain": jnp.clip(jax.random.uniform(seeds[5], (HEADS,), jnp.float32, 0.5, 1.5), 0.5, 1.5),
    }


highest = lax.Precision.HIGHEST

def state_mixer(columns, step_bias, decay_log, skip_gain, initial):
    length = columns.shape[0]
    blocks = length // GROUP
    values = jax.nn.silu(columns[:, :INNER])
    input_map = jax.nn.silu(columns[:, INNER:INNER + STATE]).reshape(blocks, GROUP, STATE)
    output_map = jax.nn.silu(columns[:, INNER + STATE:INNER + 2 * STATE]).reshape(blocks, GROUP, STATE)
    step_size = jax.nn.softplus(columns[:, INNER + 2 * STATE:] + step_bias)
    log_decay = -jnp.exp(decay_log) * step_size
    head_values = values.reshape(blocks, GROUP, HEADS, HEAD_DIM)
    scaled = head_values * step_size.reshape(blocks, GROUP, HEADS)[:, :, :, None]
    cumulative = jnp.cumsum(log_decay.reshape(blocks, GROUP, HEADS), axis=1)
    causal = (lax.broadcasted_iota(jnp.int32, (GROUP, GROUP), 0) >= lax.broadcasted_iota(jnp.int32, (GROUP, GROUP), 1))[None, :, :, None]
    differences = cumulative[:, :, None, :] - cumulative[:, None, :, :]
    within = jnp.where(causal, jnp.exp(jnp.where(causal, differences, 0.0)), 0.0)
    scores = jnp.einsum('kqn,ksn->kqs', output_map, input_map, precision=highest)
    inside = jnp.einsum('kqsh,kshp->kqhp', scores[:, :, :, None] * within, scaled, precision=highest)
    tail_decay = jnp.exp(cumulative[:, -1:, :] - cumulative)
    group_states = jnp.einsum('kshp,ksn->khpn', scaled * tail_decay[:, :, :, None], input_map, precision=highest)
    totals = cumulative[:, -1, :]

    def advance(running, inputs):
        block_total, block_state = inputs
        return (jnp.exp(block_total)[:, None, None] * running + block_state, running)
    final_state, entering = lax.scan(advance, initial, (totals, group_states))
    from_state = jnp.einsum('kqn,khpn->kqhp', output_map, entering, precision=highest) * jnp.exp(cumulative)[:, :, :, None]
    mixed_out = inside + from_state + skip_gain[None, None, :, None] * head_values
    return (mixed_out.reshape(length, INNER), final_state, lax.optimization_barrier(jnp.sum(totals, axis=0)))

def reference(hidden, output_grad, input_weight, step_bias, decay_log, skip_gain):
    initial = jnp.zeros((HEADS, HEAD_DIM, STATE), jnp.float32)

    def one_sequence(running, inputs):
        weight_sum, head_sum = running
        tokens, cotangent = inputs
        projected = jnp.dot(tokens, input_weight, preferred_element_type=jnp.float32)

        def forward(columns, bias_part, log_part, gain_part):
            return state_mixer(columns, bias_part, log_part, gain_part, initial)[0]
        unused, pullback = jax.vjp(forward, projected, step_bias, decay_log, skip_gain)
        column_grad, bias_grad, log_grad, gain_grad = pullback(cotangent.astype(jnp.float32))
        rounded = column_grad.astype(jnp.bfloat16)
        token_grad = lax.dot_general(rounded, input_weight, (((1,), (1,)), ((), ())), preferred_element_type=jnp.float32).astype(jnp.bfloat16)
        weight_sum = weight_sum + lax.dot_general(tokens, rounded, (((0,), (0,)), ((), ())), preferred_element_type=jnp.float32)
        head_sum = head_sum + jnp.stack([bias_grad, log_grad, gain_grad])
        return ((weight_sum, head_sum), token_grad)
    starting = (jnp.zeros((D, PROJ), jnp.float32), jnp.zeros((3, HEADS), jnp.float32))
    (weight_grad, head_grads), hidden_grad = lax.scan(one_sequence, starting, (hidden, output_grad))
    return (hidden_grad, weight_grad, head_grads)
```

```python
import jax
import jax.numpy as jnp
from jax import lax
from jax.experimental import pallas as pl
from jax.experimental.pallas import tpu as pltpu
from jax.sharding import Mesh
from jax.sharding import PartitionSpec as P

D = 1280
HEAD_DIM = 64
STATE = 128
INNER = 2560
NH = 5
COLS = 320
MAPS = 32
USED = COLS + MAPS + NH
WIDE = 384
SEGS = 4
SPAN = 256
ROWS = 160
ZERO = ("x", "zh")
GROUP = ("y", "c")
PEERS = ("zl", "x", "zh")


f32 = jnp.float32
bf16 = jnp.bfloat16
highest = lax.Precision.HIGHEST


def dot(a, b, dims):
    return lax.dot_general(a, b, (dims, ((), ())), preferred_element_type=f32)


def pieces(v):
    hi = v.astype(bf16)
    rest = v - hi.astype(f32)
    mid = rest.astype(bf16)
    low = (rest - mid.astype(f32)).astype(bf16)
    return hi, mid, low


def swap(v, axis="c"):
    return lax.ppermute(v, axis, [(0, 1), (1, 0)])


def along_y(v, d):
    return lax.ppermute(v, "y", [(i, (i + d) % 4) for i in range(4)])


def by_core(own, other, core, axis):
    return jnp.where(
        core == 0, jnp.concatenate([own, other], axis), jnp.concatenate([other, own], axis)
    )


def by_row(blocks, row):
    out = jnp.zeros((len(blocks),) + blocks[0].shape, blocks[0].dtype)
    for d, block in enumerate(blocks):
        out = lax.dynamic_update_index_in_dim(out, block, (row - d) % 4, 0)
    return out


TILES = ((0, 128, (0, 1)), (128, 128, (2, 3)), (256, 64, (4,)))


def halves(v):
    hi = v.astype(bf16)
    return hi, (v - hi.astype(f32)).astype(bf16)


def dot3(a, b, dims):
    ah, al = halves(a)
    bh, bl = halves(b)
    return dot(ah, bh, dims) + dot(al, bh, dims) + dot(ah, bl, dims)


def dot2(a, b, dims):
    ah, al = halves(a)
    return dot(ah, b, dims) + dot(al, b, dims)


def exact_sum(matrix, v, dims):
    return sum(dot(matrix, p, dims) for p in pieces(v))


def lanes(shape):
    return lax.broadcasted_iota(jnp.int32, shape, 1)


def low_triangle():
    return lax.broadcasted_iota(jnp.int32, (SPAN, SPAN), 0) >= lanes((SPAN, SPAN))


def spread(v, width, heads):
    if len(heads) == 1:
        return jnp.broadcast_to(v[:, heads[0]:heads[0] + 1], (v.shape[0], width))
    first, second = heads
    return jnp.where(
        lanes((v.shape[0], width)) < HEAD_DIM, v[:, first:first + 1], v[:, second:second + 1]
    )


def gathered(v, width, heads):
    row = lax.broadcasted_iota(jnp.int32, (width, 128), 0)
    pick = (heads[0] + row // HEAD_DIM == lanes((width, 128))).astype(bf16)
    return dot2(v, pick, ((1,), (0,)))


def step_of(tile, params):
    return pltpu.roll(tile, 32, 1) + params[0:1]


def softplus(v):
    return jnp.maximum(v, 0.0) + jnp.log1p(jnp.exp(-jnp.abs(v)))


def sigmoid(v):
    return 1.0 / (1.0 + jnp.exp(-v))


def silu(v):
    return v * sigmoid(v)


def forward_kernel(tokens, w, cot, params, projected, cum_out, states, sends, totals):
    k = pl.program_id(0)
    proj = dot(tokens[...], w[...], ((1,), (0,)))
    projected[...] = proj
    step = softplus(step_of(proj[:, 256:384], params))
    log_decay = step * params[1:2]
    cum = exact_sum(low_triangle().astype(bf16), log_decay, ((1,), (0,)))
    cum_out[...] = cum
    total = cum[SPAN - 1:SPAN]
    totals[pl.ds(k, 1), :] = total
    head_in = jnp.exp(cum)
    head_out = jnp.exp(total - cum) * step
    in_map = halves(silu(proj[:, WIDE:WIDE + STATE]))
    out_map = halves(silu(proj[:, WIDE + STATE:]))
    for start, width, heads in TILES:
        cols = slice(start, start + width)
        scaled_out = silu(proj[:, cols]) * spread(head_out, width, heads)
        cot_in = cot[:, cols].astype(f32) * spread(head_in, width, heads)
        for i, v, m in ((0, scaled_out, in_map), (1, cot_in, out_map)):
            hi, lo = halves(v)
            dims = ((0,), (0,))
            r = dot(hi, m[0], dims) + dot(lo, m[0], dims) + dot(hi, m[1], dims)
            states[i, cols] = r
            sends[i, cols] = r.astype(bf16)


def inside_kernel(projected, cum_in, cot, params, out_inside, grad_inside, score_grad):
    cum = cum_in[...]
    cum_t = cum.T
    step = softplus(step_of(projected[:, 256:384], params))
    in_map = silu(projected[:, WIDE:WIDE + STATE])
    out_map = silu(projected[:, WIDE + STATE:])
    scores = dot3(out_map, in_map, ((1,), (1,)))
    causal = low_triangle()
    total_grad = jnp.zeros((SPAN, SPAN), f32)
    for start, width, heads in TILES:
        cols = slice(start, start + width)
        scaled = silu(projected[:, cols]) * spread(step, width, heads)
        cot_tile = cot[:, cols]
        out = jnp.zeros((SPAN, width), f32)
        grad = jnp.zeros((SPAN, width), f32)
        for n, h in enumerate(heads):
            within = jnp.exp(jnp.where(causal, cum[:, h:h + 1] - cum_t[h:h + 1], -1e30))
            wh, wl = halves(within * scores)
            if len(heads) == 1:
                u, g = scaled, cot_tile
            else:
                mine = (lanes((SPAN, width)) < HEAD_DIM) == (n == 0)
                u = jnp.where(mine, scaled, 0.0)
                g = jnp.where(mine, cot_tile, jnp.zeros_like(cot_tile))
            uh, ul = halves(u)
            dims = ((1,), (0,))
            out += dot(wh, uh, dims) + dot(wl, uh, dims) + dot(wh, ul, dims)
            dims = ((0,), (0,))
            grad += dot(wh, g, dims) + dot(wl, g, dims)
            dims = ((1,), (1,))
            total_grad += (dot(cot_tile, uh, dims) + dot(cot_tile, ul, dims)) * within
        out_inside[:, cols] = out
        grad_inside[:, cols] = grad
    score_grad[...] = total_grad


def scan_states(later, states, got, totals, got_totals, enter, leave):
    for h in range(NH):
        rows = slice(h * HEAD_DIM, (h + 1) * HEAD_DIM)
        for i, target, order in ((0, enter, range(SEGS)), (1, leave, reversed(range(SEGS)))):
            other_first = later if i == 0 else not later
            carry = jnp.zeros((HEAD_DIM, STATE), f32)
            for k in order:
                at = slice(k * COLS + rows.start, k * COLS + rows.stop)
                own_step = (jnp.exp(totals[k:k + 1, h:h + 1]), states[i, at])
                other_step = (jnp.exp(got_totals[k:k + 1, h:h + 1]), got[i, at].astype(f32))
                if other_first:
                    carry = other_step[0] * carry + other_step[1]
                target[at] = carry
                carry = own_step[0] * carry + own_step[1]
                if not other_first:
                    carry = other_step[0] * carry + other_step[1]


def backward_kernel(
    where, projected, cum_in, cot, params, out_inside, grad_inside, score_grad,
    states, got, totals, got_totals, rounded, map_part, heads_out, enter, leave
):
    k = pl.program_id(0)
    for later in (False, True):
        @pl.when((k == 0) & (where[0] == int(later)))
        def _():
            scan_states(later, states, got, totals, got_totals, enter, leave)

    @pl.when(k == 0)
    def _():
        heads_out[...] = jnp.zeros_like(heads_out)

    cum = cum_in[...]
    total = cum[SPAN - 1:SPAN]
    raw_step = step_of(projected[:, 256:384], params)
    step = softplus(raw_step)
    rate = params[1:2]
    log_decay = step * rate
    head_in = jnp.exp(cum)
    tail = jnp.exp(total - cum)
    in_map = silu(projected[:, WIDE:WIDE + STATE])
    out_map = silu(projected[:, WIDE + STATE:])
    in_halves, out_halves = halves(in_map), halves(out_map)
    total_exp = jnp.exp(total)
    lane = lanes((1, 128))
    cum_grad = jnp.zeros((SPAN, 128), f32)
    step_grad = jnp.zeros((SPAN, 128), f32)
    last = jnp.zeros((1, 128), f32)
    skip_grad = jnp.zeros((1, 128), f32)
    in_grad = dot3(out_map, score_grad[...], ((0,), (0,)))
    out_grad = dot3(in_map, score_grad[...], ((0,), (1,)))
    step_tile = None
    value_tiles = []
    for start, width, heads in TILES:
        cols = slice(start, start + width)
        rows = pl.ds(k * COLS + start, width)
        e, l = enter[rows, :], leave[rows, :]
        eh, el = halves(e)
        lh, ll = halves(l)
        dims = ((1,), (1,))
        from_state = dot(out_halves[0], eh, dims) + dot(out_halves[1], eh, dims) + dot(out_halves[0], el, dims)
        to_state = dot(in_halves[0], lh, dims) + dot(in_halves[1], lh, dims) + dot(in_halves[0], ll, dims)
        raw = projected[:, cols]
        gate = sigmoid(raw)
        values = raw * gate
        wide_step = spread(step, width, heads)
        wide_tail = spread(tail, width, heads)
        wide_in = spread(head_in, width, heads)
        scaled = values * wide_step
        g = cot[:, cols].astype(f32)
        scaled_grad = grad_inside[:, cols] + to_state * wide_tail
        out_all = out_inside[:, cols] + from_state * wide_in
        value_grad = scaled_grad * wide_step + params[2 + start // 128:3 + start // 128, :width] * g
        value_tiles.append((cols, (value_grad * (gate * (1.0 + raw * (1.0 - gate)))).astype(bf16)))
        cum_grad += gathered(g * out_all - scaled * scaled_grad, width, heads)
        step_grad += gathered(scaled_grad * values, width, heads)
        sh, sl = halves(scaled * wide_tail)
        ch, cl = halves(g * wide_in)
        dims = ((0,), (1,))
        in_grad += dot(lh, sh, dims) + dot(ll, sh, dims) + dot(lh, sl, dims)
        out_grad += dot(eh, ch, dims) + dot(el, ch, dims) + dot(eh, cl, dims)
        skip_row = jnp.sum(g * values, axis=0, keepdims=True)
        for n, h in enumerate(heads):
            part = slice(n * HEAD_DIM, (n + 1) * HEAD_DIM)
            final = total_exp[:, h:h + 1] * e[part] + states[0, pl.ds(k * COLS + h * HEAD_DIM, HEAD_DIM), :]
            product = jnp.sum(jnp.sum(l[part] * final, axis=0, keepdims=True), axis=1, keepdims=True)
            last += jnp.where(lane == h, product, 0.0)
            mine = lanes((1, width)) // HEAD_DIM == n
            product = jnp.sum(jnp.where(mine, skip_row, 0.0), axis=1, keepdims=True)
            skip_grad += jnp.where(lane == h, product, 0.0)
    decay_grad = exact_sum(low_triangle().astype(bf16), cum_grad, ((0,), (0,))) + last
    step_grad += decay_grad * rate
    raw_step_grad = jnp.where(lanes((SPAN, 128)) < NH, step_grad * sigmoid(raw_step), 0.0)
    rounded[:, 256:384] = pltpu.roll(raw_step_grad, 96, 1).astype(bf16)
    for cols, v in value_tiles:
        rounded[:, cols] = v
    map_part[0:STATE, :] = in_grad.astype(bf16)
    map_part[STATE:, :] = out_grad.astype(bf16)
    heads_out[0:1, :] += jnp.sum(raw_step_grad, axis=0, keepdims=True)
    heads_out[1:2, :] += jnp.sum(decay_grad * log_decay, axis=0, keepdims=True)
    heads_out[2:3, :] += skip_grad


def outer_kernel(where, rounded_in, map_parts, projected, w, rounded, kept, given):
    raw = projected[...]
    gate = sigmoid(raw)
    total = jnp.sum(map_parts[...].astype(f32), axis=0)
    zero = jnp.zeros((32, SPAN), f32)
    total = jnp.concatenate([zero, zero, total, zero], axis=0).T
    total = total * (gate * (1.0 + raw * (1.0 - gate)))
    lane = lanes((SPAN, 128))
    own = (lane >= COLS - 256) & (lane < COLS - 256 + MAPS)
    tile = jnp.where(own, total.astype(bf16), rounded_in[:, 256:384])
    rounded[:, :256] = rounded_in[:, :256]
    rounded[:, 256:384] = tile
    out = dot(rounded[...], w[...], ((1,), (1,)))
    for core in (0, 1):
        @pl.when(where[0] == core)
        def _():
            kept[0] = out[core * 128:core * 128 + 128]
            given[0] = out[(1 - core) * 128:(1 - core) * 128 + 128].astype(bf16)


def call(kernel, outs, ins, scratch=()):
    def spec(block, index):
        if block is None:
            return pl.BlockSpec(memory_space=pltpu.SMEM)
        return pl.BlockSpec(block, index)

    return pl.pallas_call(
        kernel,
        grid=(SEGS,),
        in_specs=[spec(block, index) for _, block, index in ins],
        out_specs=[spec(block, index) for _, block, index in outs],
        out_shape=[shape for shape, _, _ in outs],
        scratch_shapes=list(scratch),
        compiler_params=pltpu.CompilerParams(
            dimension_semantics=("arbitrary",), vmem_limit_bytes=48 * 1024 * 1024
        ),
    )(*[v for v, _, _ in ins])


def whole(v):
    zeros = (0,) * len(v.shape)
    return (v, v.shape, lambda k: zeros)


def rows_of(v):
    return (v, (v.shape[0] // SEGS,) + v.shape[1:], lambda k: (k, 0))


def array(*dims, dtype=f32):
    return jax.ShapeDtypeStruct(dims, dtype)


def body(hidden, output_grad, input_weight, step_bias, decay_log, skip_gain):
    core = lax.axis_index("c")
    row = lax.axis_index("y")
    part_z = lax.axis_index("zl")
    group = lax.axis_index(GROUP)

    w = input_weight
    w = jnp.concatenate(
        [
            lax.dynamic_slice(w, (0, group * COLS), (ROWS, COLS)),
            lax.dynamic_slice(w, (0, INNER + group * MAPS), (ROWS, MAPS)),
            lax.dynamic_slice(w, (0, INNER + 2 * STATE + group * NH), (ROWS, NH)),
            jnp.zeros((ROWS, WIDE - USED), bf16),
            w[:, INNER:INNER + 2 * STATE],
        ],
        axis=1,
    )
    wide = WIDE + 2 * STATE
    w = lax.all_to_all(jnp.broadcast_to(w[None], (8, ROWS, wide)), ZERO, 0, 0, tiled=True)
    w = w.reshape(D, wide)

    own = hidden[0]
    tokens = by_row([own] + [along_y(own, d) for d in range(1, 4)], row)
    tokens = by_core(tokens, swap(tokens), core, 1).reshape(SEGS * SPAN, D)
    cot = output_grad[0]
    parts = []
    for d in range(4):
        part = lax.dynamic_slice(cot, (0, ((row + d) % 4) * 2 * COLS), (128, 2 * COLS))
        parts.append(along_y(part, d) if d else part)
    parts = by_row(parts, row)
    kept = lax.dynamic_slice(parts, (0, 0, core * COLS), (SEGS, 128, COLS))
    given = lax.dynamic_slice(parts, (0, 0, (1 - core) * COLS), (SEGS, 128, COLS))
    cot = by_core(kept, swap(given), core, 1)

    cot = cot.reshape(SEGS * SPAN, COLS)
    bias = lax.dynamic_slice(step_bias, (group * NH,), (NH,))
    rate = -jnp.exp(lax.dynamic_slice(decay_log, (group * NH,), (NH,)))
    skip = jnp.repeat(lax.dynamic_slice(skip_gain, (group * NH,), (NH,)), HEAD_DIM)
    params = jnp.concatenate(
        [
            jnp.pad(bias, (0, 128 - NH))[None],
            jnp.pad(rate, (0, 128 - NH))[None],
            jnp.pad(skip, (0, 64)).reshape(3, 128),
            jnp.zeros((3, 128), f32),
        ]
    )

    order = jnp.arange(D).reshape(4, 2, 2, 8, 10).transpose(1, 3, 0, 2, 4).reshape(D)
    picks = (jnp.arange(D)[:, None] == order[None, :]).astype(bf16)
    ordered = dot(picks, tokens, ((0,), (1,))).astype(bf16)

    positions = SEGS * SPAN
    count = SEGS * COLS
    projected, cum, states, sends, totals = call(
        forward_kernel,
        [
            rows_of(array(positions, wide)),
            rows_of(array(positions, 128)),
            (array(2, count, STATE), (2, COLS, STATE), lambda k: (0, k, 0)),
            (array(2, count, STATE, dtype=bf16), (2, COLS, STATE), lambda k: (0, k, 0)),
            whole(array(8, 128)),
        ],
        [rows_of(tokens), whole(w), rows_of(cot), whole(params)],
    )
    got = swap(sends, "zl")
    got_totals = swap(totals, "zl")
    out_inside, grad_inside, score_grad = call(
        inside_kernel,
        [
            rows_of(array(positions, COLS)),
            rows_of(array(positions, COLS)),
            rows_of(array(positions, SPAN)),
        ],
        [rows_of(projected), rows_of(cum), rows_of(cot), whole(params)],
    )
    rounded, map_part, heads = call(
        backward_kernel,
        [
            rows_of(array(positions, WIDE, dtype=bf16)),
            (array(2 * STATE, positions, dtype=bf16), (2 * STATE, SPAN), lambda k: (0, k)),
            whole(array(8, 128)),
        ],
        [
            (part_z.reshape(1), None, None),
            rows_of(projected),
            rows_of(cum),
            rows_of(cot),
            whole(params),
            rows_of(out_inside),
            rows_of(grad_inside),
            rows_of(score_grad),
            whole(states),
            whole(got),
            whole(totals),
            whole(got_totals),
        ],
        [pltpu.VMEM((count, STATE), f32)] * 2,
    )
    map_part = lax.all_to_all(map_part.reshape(8, MAPS, positions), GROUP, 0, 0, tiled=True)
    heads = heads[:3, :NH]

    rounded, kept, given = call(
        outer_kernel,
        [
            rows_of(array(positions, WIDE, dtype=bf16)),
            (array(SEGS, 128, D), (1, 128, D), lambda k: (k, 0, 0)),
            (array(SEGS, 128, D, dtype=bf16), (1, 128, D), lambda k: (k, 0, 0)),
        ],
        [
            (core.reshape(1), None, None),
            rows_of(rounded),
            (map_part, (8, MAPS, SPAN), lambda k: (0, 0, k)),
            (projected, (SPAN, 128), lambda k: (k, 2)),
            (w, (D, WIDE), lambda k: (0, 0)),
        ],
    )
    token_part = kept + swap(given).astype(f32)
    weight_part = dot(ordered, rounded, ((1,), (0,))).reshape(16, 80, WIDE)
    token_part, weight_part = lax.optimization_barrier((token_part, weight_part))
    token_grad = lax.dynamic_index_in_dim(token_part, row, 0, keepdims=False)
    token_part = token_part.astype(bf16)
    for d in range(1, 4):
        part = lax.dynamic_index_in_dim(token_part, (row + d) % 4, 0, keepdims=False)
        token_grad = token_grad + along_y(part, d).astype(f32)
    token_grad = token_grad.astype(bf16)

    def with_heads(part, head_rows, at):
        flat = jnp.pad(head_rows.reshape(3 * NH), (USED, WIDE - USED - 3 * NH))
        hi, mid, low = pieces(flat)
        row = lax.broadcasted_iota(jnp.int32, part.shape, part.ndim - 2)
        col = lax.broadcasted_iota(jnp.int32, part.shape, part.ndim - 1)
        part = jnp.where((row == at) & (col >= USED), hi.astype(f32), part)
        return jnp.where((row == at + 1) & (col >= USED), mid.astype(f32), part)

    part = lax.all_to_all(with_heads(weight_part, heads, 0).astype(bf16), PEERS, 0, 0, tiled=True)
    part = part.astype(f32).sum(0)
    heads = (part[0] + part[1])[USED:USED + 3 * NH]
    part = jnp.pad(part.reshape(8, 10, WIDE), ((0, 0), (0, 6), (0, 0)))
    part = lax.all_to_all(with_heads(part, heads, 10), GROUP, 0, 0, tiled=True)
    heads = (part[:, 10] + part[:, 11])[:, USED:USED + 3 * NH].reshape(8, 3, NH)
    head_grads = heads.transpose(1, 0, 2).reshape(3, 8 * NH)
    part = part[:, :10].transpose(1, 0, 2)
    weight_grad = jnp.concatenate(
        [
            part[:, :, :COLS].reshape(10, 8 * COLS),
            part[:, :, COLS:COLS + MAPS].reshape(10, 8 * MAPS),
            part[:, :, COLS + MAPS:USED].reshape(10, 8 * NH),
        ],
        axis=1,
    )
    return token_grad[None], weight_grad, head_grads


def solution(mesh):
    torus = Mesh(mesh.devices.reshape(4, 2, 2, 4, 2), ("y", "zl", "c", "x", "zh"))
    seq = ("y", "zl", "c")
    in_specs = (P(ZERO, seq, None), P(ZERO, seq, None), P(ZERO, None), P(), P(), P())
    out_specs = (P(ZERO, seq, None), P(seq + ZERO, None), P())
    return jax.shard_map(body, mesh=torus, in_specs=in_specs, out_specs=out_specs, check_vma=False)
```

```python
import jax
import jax.numpy as jnp
from jax import lax
from jax.experimental import pallas as pl
from jax.experimental.pallas import tpu as pltpu
from jax.sharding import Mesh
from jax.sharding import PartitionSpec as P

D = 1280
HEAD_DIM = 64
STATE = 128
INNER = 2560
NH = 5
COLS = 320
MAPS = 32
USED = COLS + MAPS + NH
WIDE = 384
HEAD_LANE = 360
SEGS = 4
SPAN = 256
ROWS = 160
ZERO = ("x", "zh")
GROUP = ("y", "c")


f32 = jnp.float32
bf16 = jnp.bfloat16


def dot(a, b, dims):
    return lax.dot_general(a, b, (dims, ((), ())), preferred_element_type=f32)


def pieces(v):
    hi = v.astype(bf16)
    rest = v - hi.astype(f32)
    mid = rest.astype(bf16)
    low = (rest - mid.astype(f32)).astype(bf16)
    return hi, mid, low


def swap(v, axis="c"):
    return lax.ppermute(v, axis, [(0, 1), (1, 0)])


def along_y(v, d):
    return lax.ppermute(v, "y", [(i, (i + d) % 4) for i in range(4)])


def by_core(own, other, core, axis):
    return jnp.where(
        core == 0, jnp.concatenate([own, other], axis), jnp.concatenate([other, own], axis)
    )


TILES = ((0, 128, (0, 1)), (128, 128, (2, 3)), (256, 64, (4,)))


def halves(v):
    hi = v.astype(bf16)
    return hi, (v - hi.astype(f32)).astype(bf16)


def dot3(a, b, dims):
    ah, al = halves(a)
    bh, bl = halves(b)
    return dot(ah, bh, dims) + dot(al, bh, dims) + dot(ah, bl, dims)


def exact_sum(matrix, v, dims):
    return sum(dot(matrix, p, dims) for p in pieces(v))


def lanes(shape):
    return lax.broadcasted_iota(jnp.int32, shape, 1)


def low_triangle():
    return lax.broadcasted_iota(jnp.int32, (SPAN, SPAN), 0) >= lanes((SPAN, SPAN))


def spread(v, width, heads):
    if len(heads) == 1:
        return jnp.broadcast_to(v[:, heads[0]:heads[0] + 1], (v.shape[0], width))
    first, second = heads
    return jnp.where(
        lanes((v.shape[0], width)) < HEAD_DIM, v[:, first:first + 1], v[:, second:second + 1]
    )


def step_of(tile, params):
    return pltpu.roll(tile, 32, 1) + params[0:1]


def softplus(v):
    return jnp.maximum(v, 0.0) + jnp.log1p(jnp.exp(-jnp.abs(v)))


def sigmoid(v):
    return 1.0 / (1.0 + jnp.exp(-v))


def silu(v):
    return v * sigmoid(v)


def select_kernel(where, w, out):
    group = where[0]

    def columns(start, width):
        tile = start // 128
        wide = w[:, pl.ds(pl.multiple_of(tile * 128, 128), width)].astype(f32)
        return pltpu.roll(wide, (width - (start - tile * 128)) % width, 1)

    lane = lanes((ROWS, 128))
    values = columns(group * COLS, 512)
    maps = w[:, INNER:INNER + 2 * STATE]
    own = maps.astype(f32)
    own = pltpu.roll(own, (2 * STATE + 64 - group * MAPS) % (2 * STATE), 1)[:, :128]
    steps = w[:, INNER + 2 * STATE:].astype(f32)
    steps = jnp.concatenate([steps, jnp.zeros((ROWS, 128 - 8 * NH), f32)], axis=1)
    steps = pltpu.roll(steps, (96 + 128 - group * NH) % 128, 1)
    last = jnp.where(
        lane < 64,
        values[:, 256:384],
        jnp.where(lane < 96, own, jnp.where(lane < 96 + NH, steps, 0.0)),
    ).astype(bf16)
    first = values[:, :256].astype(bf16)
    for k in range(8):
        out[k, :, :256] = first
        out[k, :, 256:384] = last
        out[k, :, 384:] = maps


def fixed_kernel(given, out):
    out[...] = given[...]


def part_kernel(where, cot, kept, given):
    core, row = where[0], where[1]
    for d in range(SEGS):
        at = pl.ds(pl.multiple_of(((row + d) % SEGS) * 2 * COLS, 128), 2 * COLS)
        wide = cot[:, at].astype(f32)
        low = wide[:, :WIDE]
        high = pltpu.roll(wide, COLS, 1)[:, :WIDE]
        kept[d] = valued(jnp.where(core == 0, low, high)).astype(bf16)
        given[d] = valued(jnp.where(core == 0, high, low)).astype(bf16)


def parted(cot, where):
    shape = (SEGS, 128, WIDE)
    return pl.pallas_call(
        part_kernel,
        grid_spec=pltpu.PrefetchScalarGridSpec(
            num_scalar_prefetch=1,
            grid=(1,),
            in_specs=[pl.BlockSpec((128, INNER), lambda k, at: (0, 0))],
            out_specs=[pl.BlockSpec(shape, lambda k, at: (0, 0, 0))] * 2,
        ),
        out_shape=[jax.ShapeDtypeStruct(shape, bf16)] * 2,
    )(where, cot)


def selected(w, group):
    return pl.pallas_call(
        select_kernel,
        grid_spec=pltpu.PrefetchScalarGridSpec(
            num_scalar_prefetch=1,
            grid=(1,),
            in_specs=[pl.BlockSpec((ROWS, 2856), lambda k, at: (0, 0))],
            out_specs=pl.BlockSpec((8, ROWS, WIDE + 2 * STATE), lambda k, at: (0, 0, 0)),
        ),
        out_shape=jax.ShapeDtypeStruct((8, ROWS, WIDE + 2 * STATE), bf16),
    )(group.reshape(1), w)


def wide_spread(v):
    lane = lanes((v.shape[0], 128))
    return jnp.concatenate(
        [
            jnp.where(lane < HEAD_DIM, v[:, 0:1], v[:, 1:2]),
            jnp.where(lane < HEAD_DIM, v[:, 2:3], v[:, 3:4]),
            jnp.where(lane < HEAD_DIM, v[:, 4:5], 0.0),
        ],
        axis=1,
    )


def valued(v):
    return jnp.where(lanes(v.shape) < COLS, v, 0.0)


def paired(a, b, dims):
    ah, al = halves(a)
    bh, bl = halves(b)
    n = b.shape[1 - dims[1][0]]
    axis = 1 - dims[1][0]
    r = dot(ah, jnp.concatenate([bh, bl], axis=axis), dims)
    return r[:, :n] + r[:, n:] + dot(al, bh, dims)


def wide_gathered(v):
    vh, vl = halves(v)
    pick = (
        lax.broadcasted_iota(jnp.int32, (WIDE, 128), 0) // HEAD_DIM == lanes((WIDE, 128))
    ).astype(bf16)
    return dot(
        jnp.concatenate([vh, vl], axis=1), jnp.concatenate([pick, pick], axis=0), ((1,), (0,))
    )


def forward_kernel(
    where, own, other, w, cot, params, projected, cum_out, states, sends, totals, tokens
):
    k = pl.program_id(0)
    core = where[0]
    tokens[pl.ds(pl.multiple_of(core * 128, 128), 128), :] = own[0]
    tokens[pl.ds(pl.multiple_of((1 - core) * 128, 128), 128), :] = other[0]
    proj = dot(tokens[...], w[...], ((1,), (0,)))
    projected[...] = proj
    step = softplus(step_of(proj[:, 256:384], params))
    log_decay = step * params[1:2]
    cum = exact_sum(low_triangle().astype(bf16), log_decay, ((1,), (0,)))
    cum_out[...] = cum
    total = cum[SPAN - 1:SPAN]
    totals[pl.ds(k, 1), :] = total
    scaled_out = silu(valued(proj[:, :WIDE])) * wide_spread(jnp.exp(total - cum) * step)
    cot_in = cot[0].astype(f32) * wide_spread(jnp.exp(cum))
    for i, v, m in ((0, scaled_out, WIDE), (1, cot_in, WIDE + STATE)):
        r = paired(v, silu(proj[:, m:m + STATE]), ((0,), (0,)))[:COLS]
        states[i] = r
        sends[i] = r.astype(bf16)


def inside_kernel(where, projected, cum_in, cot, params, out_inside, grad_inside, map_inside):
    cum = cum_in[...]
    cum_t = cum.T
    step = softplus(step_of(projected[:, 256:384], params))
    in_map = silu(projected[:, WIDE:WIDE + STATE])
    out_map = silu(projected[:, WIDE + STATE:])
    scores = dot3(out_map, in_map, ((1,), (1,)))
    causal = low_triangle()
    total_grad = jnp.zeros((SPAN, SPAN), f32)
    for start, width, heads in TILES:
        cols = slice(start, start + width)
        scaled = silu(projected[:, cols]) * spread(step, width, heads)
        cot_tile = cot[0, :, cols]
        out = jnp.zeros((SPAN, width), f32)
        grad = jnp.zeros((SPAN, width), f32)
        for n, h in enumerate(heads):
            within = jnp.exp(jnp.where(causal, cum[:, h:h + 1] - cum_t[h:h + 1], -1e30))
            wh, wl = halves(within * scores)
            if len(heads) == 1:
                u, g = scaled, cot_tile
            else:
                mine = (lanes((SPAN, width)) < HEAD_DIM) == (n == 0)
                u = jnp.where(mine, scaled, 0.0)
                g = jnp.where(mine, cot_tile, jnp.zeros_like(cot_tile))
            uh, ul = halves(u)
            dims = ((1,), (0,))
            out += dot(wh, uh, dims) + dot(wl, uh, dims) + dot(wh, ul, dims)
            dims = ((0,), (0,))
            grad += dot(wh, g, dims) + dot(wl, g, dims)
            dims = ((1,), (1,))
            total_grad += (dot(cot_tile, uh, dims) + dot(cot_tile, ul, dims)) * within
        out_inside[:, cols] = out
        grad_inside[:, cols] = grad
    out_inside[:, COLS:] = jnp.zeros((SPAN, WIDE - COLS), f32)
    grad_inside[:, COLS:] = jnp.zeros((SPAN, WIDE - COLS), f32)
    map_inside[:, :STATE] = paired(total_grad, out_map, ((0,), (0,)))
    map_inside[:, STATE:] = paired(total_grad, in_map, ((1,), (0,)))


def scan_states(later, own, got, i, totals, got_totals, target, forward):
    other_first = later if forward else not later
    for h in range(NH):
        carry = jnp.zeros((HEAD_DIM, STATE), f32)
        for k in range(SEGS) if forward else reversed(range(SEGS)):
            at = slice(k * COLS + h * HEAD_DIM, k * COLS + (h + 1) * HEAD_DIM)
            own_step = (jnp.exp(totals[k:k + 1, h:h + 1]), own[i, at])
            other_step = (jnp.exp(got_totals[k:k + 1, h:h + 1]), got[i, at].astype(f32))
            if other_first:
                carry = other_step[0] * carry + other_step[1]
            target[k * WIDE + h * HEAD_DIM:k * WIDE + (h + 1) * HEAD_DIM] = carry
            carry = own_step[0] * carry + own_step[1]
            if not other_first:
                carry = other_step[0] * carry + other_step[1]


def backward_kernel(
    where, projected, cum_in, cot, params, out_inside, grad_inside, map_inside, states,
    got, totals, got_totals, rounded, map_part, heads_out, enter, leave
):
    k = pl.program_id(0)
    for later in (False, True):
        @pl.when((k == 0) & (where[2] == int(later)))
        def _():
            scan_states(later, states, got, 0, totals, got_totals, enter, True)
            scan_states(later, states, got, 1, totals, got_totals, leave, False)

    @pl.when(k == 0)
    def _():
        heads_out[...] = jnp.zeros_like(heads_out)
        for i in range(SEGS):
            enter[i * WIDE + COLS:(i + 1) * WIDE] = jnp.zeros((WIDE - COLS, STATE), f32)
            leave[i * WIDE + COLS:(i + 1) * WIDE] = jnp.zeros((WIDE - COLS, STATE), f32)

    cum = cum_in[...]
    total = cum[SPAN - 1:SPAN]
    raw_step = step_of(projected[:, 256:384], params)
    step = softplus(raw_step)
    rate = params[1:2]
    log_decay = step * rate
    in_map = silu(projected[:, WIDE:WIDE + STATE])
    out_map = silu(projected[:, WIDE + STATE:])
    rows = pl.ds(pl.multiple_of(k * WIDE, WIDE), WIDE)
    e, l = enter[rows, :], leave[rows, :]

    def from_map(m, v):
        mh, ml = halves(m)
        vh, vl = halves(v)
        return dot(
            jnp.concatenate([mh, ml, mh], axis=1),
            jnp.concatenate([vh, vh, vl], axis=1),
            ((1,), (1,)),
        )

    raw = valued(projected[:, :WIDE])
    gate = sigmoid(raw)
    values = raw * gate
    wide_step = wide_spread(step)
    wide_tail = wide_spread(jnp.exp(total - cum))
    wide_in = wide_spread(jnp.exp(cum))
    scaled = values * wide_step
    g = cot[0].astype(f32)
    scaled_grad = grad_inside[...] + from_map(in_map, l) * wide_tail
    out_all = out_inside[...] + from_map(out_map, e) * wide_in
    skip = jnp.concatenate([params[2:3], params[3:4], params[4:5]], axis=1)
    value_grad = scaled_grad * wide_step + skip * g
    raw_value_grad = value_grad * (gate * (1.0 + raw * (1.0 - gate)))
    cum_grad = wide_gathered(g * out_all - scaled * scaled_grad)
    step_grad = wide_gathered(scaled_grad * values)
    in_grad = paired(scaled * wide_tail, l, ((1,), (0,))) + map_inside[:, :STATE]
    out_grad = paired(g * wide_in, e, ((1,), (0,))) + map_inside[:, STATE:]
    lane = lanes((1, 128))
    total_exp = jnp.exp(total)
    skip_row = jnp.broadcast_to(jnp.sum(g * values, axis=0, keepdims=True), (8, WIDE))
    skip_grad = wide_gathered(skip_row)[0:1]
    last = jnp.zeros((1, 128), f32)
    for h in range(NH):
        part = slice(h * HEAD_DIM, (h + 1) * HEAD_DIM)
        own = states[0, pl.ds(k * COLS + h * HEAD_DIM, HEAD_DIM), :]
        product = l[part] * (total_exp[:, h:h + 1] * e[part] + own)
        product = jnp.sum(jnp.sum(product, axis=0, keepdims=True), axis=1, keepdims=True)
        last += jnp.where(lane == h, product, 0.0)
    decay_grad = exact_sum(low_triangle().astype(bf16), cum_grad, ((0,), (0,))) + last
    step_grad += decay_grad * rate
    raw_step_grad = jnp.where(lanes((SPAN, 128)) < NH, step_grad * sigmoid(raw_step), 0.0)
    rounded[:, :256] = raw_value_grad[:, :256].astype(bf16)
    rounded[:, 256:384] = (raw_value_grad[:, 256:384] + pltpu.roll(raw_step_grad, 96, 1)).astype(bf16)
    map_part[0:STATE, :] = in_grad.T.astype(bf16)
    map_part[STATE:, :] = out_grad.T.astype(bf16)
    heads_out[0:1, :] += jnp.sum(raw_step_grad, axis=0, keepdims=True)
    heads_out[1:2, :] += jnp.sum(decay_grad * log_decay, axis=0, keepdims=True)
    heads_out[2:3, :] += skip_grad


def weight_kernel(rounded, ordered, total):
    part = dot(ordered[...], rounded[...], ((1,), (0,)))
    k = pl.program_id(0)

    @pl.when(k == 0)
    def _():
        total[...] = part

    @pl.when(k > 0)
    def _():
        total[...] += part


def map_kernel(rounded_in, map_parts, projected, ordered, heads, partial, rounded, weight_out, total):
    k = pl.program_id(0)
    raw = projected[...]
    gate = sigmoid(raw)
    maps = jnp.sum(map_parts[...].astype(f32), axis=0)
    zero = jnp.zeros((32, SPAN), f32)
    maps = jnp.concatenate([zero, zero, maps, zero], axis=0).T
    maps = maps * (gate * (1.0 + raw * (1.0 - gate)))
    lane = lanes((SPAN, 128))
    own = (lane >= COLS - 256) & (lane < COLS - 256 + MAPS)
    maps = jnp.where(own, maps, 0.0).astype(bf16)
    rounded[:, :256] = rounded_in[:, :256]
    rounded[:, 256:384] = jnp.where(own, maps, rounded_in[:, 256:384])
    part = dot(ordered[...], maps, ((1,), (0,)))

    @pl.when(k == 0)
    def _():
        total[...] = partial[:, 256:384] + part

    @pl.when(k > 0)
    def _():
        total[...] += part

    @pl.when(k == SEGS - 1)
    def _():
        sums = jnp.zeros((1, 128), f32)
        for i in range(3):
            sums += pltpu.roll(
                jnp.where(lanes((1, 128)) < NH, heads[i:i + 1], 0.0), HEAD_LANE + i * NH - 256, 1
            )
        hi, lo = halves(sums)
        row = lax.broadcasted_iota(jnp.int32, (8, 128), 0)
        extra = jnp.where(row == 0, hi.astype(f32), jnp.where(row == 1, lo.astype(f32), 0.0))
        row = lax.broadcasted_iota(jnp.int32, (128, 128), 0)
        owner, slot = row // 32, row % 32
        source = jnp.where(
            slot < 30, (slot // 10) * 40 + owner * 10 + slot % 10, slot + 90
        )
        pick = (source == lanes((128, 128))).astype(bf16)

        def four_owners(i, carry):
            at = pl.ds(pl.multiple_of(i * 40, 8), 40)
            tiles = [partial[at, :128], partial[at, 128:256], total[at, :]]
            block = jnp.concatenate(tiles + [extra], axis=0).astype(bf16)
            out = dot(pick, block, ((1,), (0,))).astype(bf16)
            weight_out[pl.ds(pl.multiple_of(i * 128, 128), 128), :] = out
            return carry

        lax.fori_loop(0, 32, four_owners, 0, unroll=8)


def token_kernel(where, rounded, w, kept, given):
    out = dot(rounded[...], w[...], ((1,), (1,)))
    for core in (0, 1):
        @pl.when(where[0] == core)
        def _():
            kept[0] = out[core * 128:core * 128 + 128]
            given[0] = out[(1 - core) * 128:(1 - core) * 128 + 128].astype(bf16)


def collect_kernel(parts, out):
    for group in range(8):
        total = jnp.zeros((32, 128), f32)
        for z in range(2):
            for i in range(8):
                total += parts[((group // 2 * 2 + z) * 2 + group % 2) * 8 + i].astype(f32)
        out[group] = total


def call(kernel, outs, ins, scratch=(), where=None):
    def spec(block, index):
        return pl.BlockSpec(block, index if index.__code__.co_argcount == 2 else lambda k, *at: index(k))

    return pl.pallas_call(
        kernel,
        grid_spec=pltpu.PrefetchScalarGridSpec(
            num_scalar_prefetch=0 if where is None else 1,
            grid=(SEGS,),
            in_specs=[spec(block, index) for _, block, index in ins],
            out_specs=[spec(block, index) for _, block, index in outs],
            scratch_shapes=list(scratch),
        ),
        out_shape=[shape for shape, _, _ in outs],
        compiler_params=pltpu.CompilerParams(
            dimension_semantics=("arbitrary",), vmem_limit_bytes=20 * 1024 * 1024
        ),
    )(*([] if where is None else [where]), *[v for v, _, _ in ins])


def whole(v):
    zeros = (0,) * len(v.shape)
    return (v, v.shape, lambda k: zeros)


def rows_of(v):
    return (v, (v.shape[0] // SEGS,) + v.shape[1:], lambda k: (k, 0))


def array(*dims, dtype=f32):
    return jax.ShapeDtypeStruct(dims, dtype)


def body(hidden, output_grad, input_weight, step_bias, decay_log, skip_gain):
    core = lax.axis_index("c")
    row = lax.axis_index("y")
    part_z = lax.axis_index("zl")
    group = lax.axis_index(GROUP)

    wide = WIDE + 2 * STATE
    w = lax.all_to_all(selected(input_weight, group), ZERO, 0, 0, tiled=True)
    w = w.reshape(D, wide)

    own = hidden[0]
    parts = [own] + [along_y(own, d) for d in range(1, 4)]
    others = jnp.stack([swap(v) for v in parts])
    owns = jnp.stack(parts)
    kept, given = parted(output_grad[0], jnp.stack([core, row]))
    given = swap(given)
    cots = []
    for d in range(SEGS):
        part = by_core(kept[d], given[d], core, 0)
        cots.append(along_y(part, d) if d else part)
    cots = jnp.stack(cots)
    bias = lax.dynamic_slice(step_bias, (group * NH,), (NH,))
    rate = -jnp.exp(lax.dynamic_slice(decay_log, (group * NH,), (NH,)))
    skip = jnp.repeat(lax.dynamic_slice(skip_gain, (group * NH,), (NH,)), HEAD_DIM)
    params = jnp.concatenate(
        [
            jnp.pad(bias, (0, 128 - NH))[None],
            jnp.pad(rate, (0, 128 - NH))[None],
            jnp.pad(skip, (0, 64)).reshape(3, 128),
            jnp.zeros((3, 128), f32),
        ]
    )

    params = pl.pallas_call(fixed_kernel, name="fixed", out_shape=array(8, 128))(params)

    positions = SEGS * SPAN
    count = SEGS * COLS

    def both(dtype):
        return (array(2, count, STATE, dtype=dtype), (2, COLS, STATE), lambda k: (0, k, 0))

    place = jnp.stack([core, row, part_z])
    placed_cot = (cots, (1, SPAN, WIDE), lambda k, at: ((at[1] + SEGS - k) % SEGS, 0, 0))
    projected, cum, states, sends, totals, tokens = call(
        forward_kernel,
        [
            rows_of(array(positions, wide)),
            rows_of(array(positions, 128)),
            both(f32),
            both(bf16),
            whole(array(8, 128)),
            rows_of(array(positions, D, dtype=bf16)),
        ],
        [
            (owns, (1, 128, D), lambda k, at: ((at[1] + SEGS - k) % SEGS, 0, 0)),
            (others, (1, 128, D), lambda k, at: ((at[1] + SEGS - k) % SEGS, 0, 0)),
            whole(w),
            placed_cot,
            whole(params),
        ],
        where=place,
    )
    got = swap(sends, "zl")
    got_totals = swap(totals, "zl")

    ordered = tokens.T

    out_inside, grad_inside, map_inside = call(
        inside_kernel,
        [
            rows_of(array(positions, WIDE)),
            rows_of(array(positions, WIDE)),
            rows_of(array(positions, SPAN)),
        ],
        [rows_of(projected), rows_of(cum), placed_cot, whole(params)],
        where=place,
    )
    rounded, map_part, heads = call(
        backward_kernel,
        [
            rows_of(array(positions, WIDE, dtype=bf16)),
            (array(2 * STATE, positions, dtype=bf16), (2 * STATE, SPAN), lambda k: (0, k)),
            whole(array(8, 128)),
        ],
        [
            rows_of(projected),
            rows_of(cum),
            placed_cot,
            whole(params),
            rows_of(out_inside),
            rows_of(grad_inside),
            rows_of(map_inside),
            whole(states),
            whole(got),
            whole(totals),
            whole(got_totals),
        ],
        [pltpu.VMEM((SEGS * WIDE, STATE), f32)] * 2,
        where=place,
    )
    map_part = lax.all_to_all(map_part.reshape(8, MAPS, positions), GROUP, 0, 0, tiled=True)
    (weight_part,) = call(
        weight_kernel,
        [whole(array(D, WIDE))],
        [rows_of(rounded), (ordered, (D, SPAN), lambda k: (0, k))],
    )

    rounded, weight_part = call(
        map_kernel,
        [rows_of(array(positions, WIDE, dtype=bf16)), whole(array(128 * 32, 128, dtype=bf16))],
        [
            rows_of(rounded),
            (map_part, (8, MAPS, SPAN), lambda k: (0, 0, k)),
            (projected, (SPAN, 128), lambda k: (k, 2)),
            (ordered, (D, SPAN), lambda k: (0, k)),
            whole(heads),
            whole(weight_part),
        ],
        [pltpu.VMEM((D, 128), f32)],
    )
    part = lax.all_to_all(
        weight_part.reshape(128, 32, 128), ("y", "zl", "c", "x", "zh"), 0, 0, tiled=True
    )
    kept, given = call(
        token_kernel,
        [
            (array(SEGS, 128, D), (1, 128, D), lambda k: (k, 0, 0)),
            (array(SEGS, 128, D, dtype=bf16), (1, 128, D), lambda k: (k, 0, 0)),
        ],
        [rows_of(rounded), (w, (D, WIDE), lambda k: (0, 0))],
        where=core.reshape(1),
    )
    other = swap(given)

    def term(d):
        at = (row + d) % 4
        a = lax.dynamic_index_in_dim(kept, at, 0, keepdims=False)
        return a + lax.dynamic_index_in_dim(other, at, 0, keepdims=False).astype(f32)

    token_grad = term(0)
    terms = [term(d).astype(bf16) for d in range(1, 4)]
    returned = [along_y(v, d) for d, v in zip(range(1, 4), terms)]
    part, *terms = lax.optimization_barrier((part, *terms))
    part = pl.pallas_call(
        collect_kernel, name="collect", out_shape=array(8, 32, 128)
    )(part)
    for v in returned:
        token_grad = token_grad + v.astype(f32)
    token_grad = token_grad.astype(bf16)
    at = HEAD_LANE - 256
    heads = (part[:, 30] + part[:, 31])[:, at:at + 3 * NH].reshape(8, 3, NH)
    head_grads = heads.transpose(1, 0, 2).reshape(3, 8 * NH)
    part = part[:, :30].reshape(8, 3, 10, 128).transpose(2, 0, 1, 3).reshape(10, 8, WIDE)
    weight_grad = jnp.concatenate(
        [
            part[:, :, :COLS].reshape(10, 8 * COLS),
            part[:, :, COLS:COLS + MAPS].reshape(10, 8 * MAPS),
            part[:, :, COLS + MAPS:USED].reshape(10, 8 * NH),
        ],
        axis=1,
    )
    return token_grad[None], weight_grad, head_grads


def solution(mesh):
    torus = Mesh(mesh.devices.reshape(4, 2, 2, 4, 2), ("y", "zl", "c", "x", "zh"))
    seq = ("y", "zl", "c")
    in_specs = (P(ZERO, seq, None), P(ZERO, seq, None), P(ZERO, None), P(), P(), P())
    out_specs = (P(ZERO, seq, None), P(seq + ZERO, None), P())
    return jax.shard_map(body, mesh=torus, in_specs=in_specs, out_specs=out_specs, check_vma=False)
```

```python
import jax
import jax.numpy as jnp
from jax import lax
from jax.experimental import pallas as pl
from jax.experimental.pallas import tpu as pltpu
from jax.sharding import Mesh
from jax.sharding import PartitionSpec as P

D = 1280
HEAD_DIM = 64
STATE = 128
INNER = 2560
NH = 5
COLS = 320
MAPS = 32
USED = COLS + MAPS + NH
WIDE = 384
HEAD_LANE = 360
SEGS = 4
SPAN = 256
ROWS = 160
ZERO = ("x", "zh")
GROUP = ("y", "c")


f32 = jnp.float32
bf16 = jnp.bfloat16


def dot(a, b, dims):
    return lax.dot_general(a, b, (dims, ((), ())), preferred_element_type=f32)


def pieces(v):
    hi = v.astype(bf16)
    rest = v - hi.astype(f32)
    mid = rest.astype(bf16)
    low = (rest - mid.astype(f32)).astype(bf16)
    return hi, mid, low


def swap(v, axis="c"):
    return lax.ppermute(v, axis, [(0, 1), (1, 0)])


def along_y(v, d):
    return lax.ppermute(v, "y", [(i, (i + d) % 4) for i in range(4)])


def by_core(own, other, core, axis):
    return jnp.where(
        core == 0, jnp.concatenate([own, other], axis), jnp.concatenate([other, own], axis)
    )


TILES = ((0, 128, (0, 1)), (128, 128, (2, 3)), (256, 64, (4,)))


def halves(v):
    hi = v.astype(bf16)
    return hi, (v - hi.astype(f32)).astype(bf16)


def dot3(a, b, dims):
    ah, al = halves(a)
    bh, bl = halves(b)
    return dot(ah, bh, dims) + dot(al, bh, dims) + dot(ah, bl, dims)


def exact_sum(matrix, v, dims):
    return sum(dot(matrix, p, dims) for p in pieces(v))


def lanes(shape):
    return lax.broadcasted_iota(jnp.int32, shape, 1)


def low_triangle():
    return lax.broadcasted_iota(jnp.int32, (SPAN, SPAN), 0) >= lanes((SPAN, SPAN))


def spread(v, width, heads):
    if len(heads) == 1:
        return jnp.broadcast_to(v[:, heads[0]:heads[0] + 1], (v.shape[0], width))
    first, second = heads
    return jnp.where(
        lanes((v.shape[0], width)) < HEAD_DIM, v[:, first:first + 1], v[:, second:second + 1]
    )


def step_of(tile, params):
    return pltpu.roll(tile, 32, 1) + params[0:1]


def softplus(v):
    return jnp.maximum(v, 0.0) + jnp.log1p(jnp.exp(-jnp.abs(v)))


def sigmoid(v):
    return 1.0 / (1.0 + jnp.exp(-v))


def silu(v):
    return v * sigmoid(v)


def select_kernel(where, w, out):
    group = where[0]

    def columns(start, width):
        tile = start // 128
        wide = w[:, pl.ds(pl.multiple_of(tile * 128, 128), width)].astype(f32)
        return pltpu.roll(wide, (width - (start - tile * 128)) % width, 1)

    lane = lanes((ROWS, 128))
    values = columns(group * COLS, 512)
    maps = w[:, INNER:INNER + 2 * STATE]
    own = maps.astype(f32)
    own = pltpu.roll(own, (2 * STATE + 64 - group * MAPS) % (2 * STATE), 1)[:, :128]
    steps = w[:, INNER + 2 * STATE:].astype(f32)
    steps = jnp.concatenate([steps, jnp.zeros((ROWS, 128 - 8 * NH), f32)], axis=1)
    steps = pltpu.roll(steps, (96 + 128 - group * NH) % 128, 1)
    last = jnp.where(
        lane < 64,
        values[:, 256:384],
        jnp.where(lane < 96, own, jnp.where(lane < 96 + NH, steps, 0.0)),
    ).astype(bf16)
    first = values[:, :256].astype(bf16)
    half = jnp.where(where[1] == 0, maps[:, :STATE], maps[:, STATE:])
    for k in range(8):
        out[k, :, :256] = first
        out[k, :, 256:384] = last
        out[k, :, 384:] = half


def fixed_kernel(given, out):
    out[...] = given[...]


def part_kernel(where, cot, kept, given):
    core, row = where[0], where[1]
    for d in range(SEGS):
        at = pl.ds(pl.multiple_of(((row + d) % SEGS) * 2 * COLS, 128), 2 * COLS)
        wide = cot[:, at].astype(f32)
        low = wide[:, :WIDE]
        high = pltpu.roll(wide, COLS, 1)[:, :WIDE]
        kept[d] = valued(jnp.where(core == 0, low, high)).astype(bf16)
        given[d] = valued(jnp.where(core == 0, high, low)).astype(bf16)


def parted(cot, where):
    shape = (SEGS, 128, WIDE)
    return pl.pallas_call(
        part_kernel,
        grid_spec=pltpu.PrefetchScalarGridSpec(
            num_scalar_prefetch=1,
            grid=(1,),
            in_specs=[pl.BlockSpec((128, INNER), lambda k, at: (0, 0))],
            out_specs=[pl.BlockSpec(shape, lambda k, at: (0, 0, 0))] * 2,
        ),
        out_shape=[jax.ShapeDtypeStruct(shape, bf16)] * 2,
    )(where, cot)


def selected(w, where):
    return pl.pallas_call(
        select_kernel,
        grid_spec=pltpu.PrefetchScalarGridSpec(
            num_scalar_prefetch=1,
            grid=(1,),
            in_specs=[pl.BlockSpec((ROWS, 2856), lambda k, at: (0, 0))],
            out_specs=pl.BlockSpec((8, ROWS, WIDE + STATE), lambda k, at: (0, 0, 0)),
        ),
        out_shape=jax.ShapeDtypeStruct((8, ROWS, WIDE + STATE), bf16),
    )(where, w)


def wide_spread(v):
    lane = lanes((v.shape[0], 128))
    return jnp.concatenate(
        [
            jnp.where(lane < HEAD_DIM, v[:, 0:1], v[:, 1:2]),
            jnp.where(lane < HEAD_DIM, v[:, 2:3], v[:, 3:4]),
            jnp.where(lane < HEAD_DIM, v[:, 4:5], 0.0),
        ],
        axis=1,
    )


def valued(v):
    return jnp.where(lanes(v.shape) < COLS, v, 0.0)


def paired(a, b, dims):
    ah, al = halves(a)
    bh, bl = halves(b)
    n = b.shape[1 - dims[1][0]]
    axis = 1 - dims[1][0]
    r = dot(ah, jnp.concatenate([bh, bl], axis=axis), dims)
    return r[:, :n] + r[:, n:] + dot(al, bh, dims)


def wide_gathered(v):
    vh, vl = halves(v)
    pick = (
        lax.broadcasted_iota(jnp.int32, (WIDE, 128), 0) // HEAD_DIM == lanes((WIDE, 128))
    ).astype(bf16)
    return dot(
        jnp.concatenate([vh, vl], axis=1), jnp.concatenate([pick, pick], axis=0), ((1,), (0,))
    )


def forward_kernel(
    where, own, other, w, w_other, cot, params, projected, cum_out, states, sends, totals, tokens
):
    k = pl.program_id(0)
    core = where[0]
    tokens[pl.ds(pl.multiple_of(core * 128, 128), 128), :] = own[0]
    tokens[pl.ds(pl.multiple_of((1 - core) * 128, 128), 128), :] = other[0]
    proj = dot(tokens[...], w[...], ((1,), (0,)))
    mine = proj[:, WIDE:]
    theirs = dot(tokens[...], w_other[...], ((1,), (0,)))
    maps = (jnp.where(core == 0, mine, theirs), jnp.where(core == 0, theirs, mine))
    projected[:, :WIDE] = proj[:, :WIDE]
    projected[:, WIDE:WIDE + STATE] = maps[0]
    projected[:, WIDE + STATE:] = maps[1]
    step = softplus(step_of(proj[:, 256:384], params))
    log_decay = step * params[1:2]
    cum = exact_sum(low_triangle().astype(bf16), log_decay, ((1,), (0,)))
    cum_out[...] = cum
    total = cum[SPAN - 1:SPAN]
    totals[pl.ds(k, 1), :] = total
    scaled_out = silu(valued(proj[:, :WIDE])) * wide_spread(jnp.exp(total - cum) * step)
    cot_in = cot[0].astype(f32) * wide_spread(jnp.exp(cum))
    for i, v in ((0, scaled_out), (1, cot_in)):
        r = paired(v, silu(maps[i]), ((0,), (0,)))[:COLS]
        states[i] = r
        sends[i] = r.astype(bf16)


def inside_kernel(where, projected, cum_in, cot, params, out_inside, grad_inside, map_inside):
    cum = cum_in[...]
    cum_t = cum.T
    step = softplus(step_of(projected[:, 256:384], params))
    in_map = silu(projected[:, WIDE:WIDE + STATE])
    out_map = silu(projected[:, WIDE + STATE:])
    scores = dot3(out_map, in_map, ((1,), (1,)))
    causal = low_triangle()
    total_grad = jnp.zeros((SPAN, SPAN), f32)
    for start, width, heads in TILES:
        cols = slice(start, start + width)
        scaled = silu(projected[:, cols]) * spread(step, width, heads)
        cot_tile = cot[0, :, cols]
        out = jnp.zeros((SPAN, width), f32)
        grad = jnp.zeros((SPAN, width), f32)
        for n, h in enumerate(heads):
            within = jnp.exp(jnp.where(causal, cum[:, h:h + 1] - cum_t[h:h + 1], -1e30))
            wh, wl = halves(within * scores)
            if len(heads) == 1:
                u, g = scaled, cot_tile
            else:
                mine = (lanes((SPAN, width)) < HEAD_DIM) == (n == 0)
                u = jnp.where(mine, scaled, 0.0)
                g = jnp.where(mine, cot_tile, jnp.zeros_like(cot_tile))
            uh, ul = halves(u)
            dims = ((1,), (0,))
            out += dot(wh, uh, dims) + dot(wl, uh, dims) + dot(wh, ul, dims)
            dims = ((0,), (0,))
            grad += dot(wh, g, dims) + dot(wl, g, dims)
            dims = ((1,), (1,))
            total_grad += (dot(cot_tile, uh, dims) + dot(cot_tile, ul, dims)) * within
        out_inside[:, cols] = out
        grad_inside[:, cols] = grad
    out_inside[:, COLS:] = jnp.zeros((SPAN, WIDE - COLS), f32)
    grad_inside[:, COLS:] = jnp.zeros((SPAN, WIDE - COLS), f32)
    map_inside[:, :STATE] = paired(total_grad, out_map, ((0,), (0,)))
    map_inside[:, STATE:] = paired(total_grad, in_map, ((1,), (0,)))


def scan_states(later, own, got, i, totals, got_totals, target, forward):
    other_first = later if forward else not later
    for h in range(NH):
        carry = jnp.zeros((HEAD_DIM, STATE), f32)
        for k in range(SEGS) if forward else reversed(range(SEGS)):
            at = slice(k * COLS + h * HEAD_DIM, k * COLS + (h + 1) * HEAD_DIM)
            own_step = (jnp.exp(totals[k:k + 1, h:h + 1]), own[i, at])
            other_step = (jnp.exp(got_totals[k:k + 1, h:h + 1]), got[i, at].astype(f32))
            if other_first:
                carry = other_step[0] * carry + other_step[1]
            target[k * WIDE + h * HEAD_DIM:k * WIDE + (h + 1) * HEAD_DIM] = carry
            carry = own_step[0] * carry + own_step[1]
            if not other_first:
                carry = other_step[0] * carry + other_step[1]


def backward_kernel(
    where, projected, cum_in, cot, params, out_inside, grad_inside, map_inside, states,
    got, totals, got_totals, rounded, map_part, heads_out, enter, leave
):
    k = pl.program_id(0)
    for later in (False, True):
        @pl.when((k == 0) & (where[2] == int(later)))
        def _():
            scan_states(later, states, got, 0, totals, got_totals, enter, True)
            scan_states(later, states, got, 1, totals, got_totals, leave, False)

    @pl.when(k == 0)
    def _():
        heads_out[...] = jnp.zeros_like(heads_out)
        for i in range(SEGS):
            enter[i * WIDE + COLS:(i + 1) * WIDE] = jnp.zeros((WIDE - COLS, STATE), f32)
            leave[i * WIDE + COLS:(i + 1) * WIDE] = jnp.zeros((WIDE - COLS, STATE), f32)

    cum = cum_in[...]
    total = cum[SPAN - 1:SPAN]
    raw_step = step_of(projected[:, 256:384], params)
    step = softplus(raw_step)
    rate = params[1:2]
    log_decay = step * rate
    in_map = silu(projected[:, WIDE:WIDE + STATE])
    out_map = silu(projected[:, WIDE + STATE:])
    rows = pl.ds(pl.multiple_of(k * WIDE, WIDE), WIDE)
    e, l = enter[rows, :], leave[rows, :]

    def from_map(m, v):
        mh, ml = halves(m)
        vh, vl = halves(v)
        return dot(
            jnp.concatenate([mh, ml, mh], axis=1),
            jnp.concatenate([vh, vh, vl], axis=1),
            ((1,), (1,)),
        )

    raw = valued(projected[:, :WIDE])
    gate = sigmoid(raw)
    values = raw * gate
    wide_step = wide_spread(step)
    wide_tail = wide_spread(jnp.exp(total - cum))
    wide_in = wide_spread(jnp.exp(cum))
    scaled = values * wide_step
    g = cot[0].astype(f32)
    scaled_grad = grad_inside[...] + from_map(in_map, l) * wide_tail
    out_all = out_inside[...] + from_map(out_map, e) * wide_in
    skip = jnp.concatenate([params[2:3], params[3:4], params[4:5]], axis=1)
    value_grad = scaled_grad * wide_step + skip * g
    raw_value_grad = value_grad * (gate * (1.0 + raw * (1.0 - gate)))
    cum_grad = wide_gathered(g * out_all - scaled * scaled_grad)
    step_grad = wide_gathered(scaled_grad * values)
    in_grad = paired(scaled * wide_tail, l, ((1,), (0,))) + map_inside[:, :STATE]
    out_grad = paired(g * wide_in, e, ((1,), (0,))) + map_inside[:, STATE:]
    lane = lanes((1, 128))
    total_exp = jnp.exp(total)
    skip_row = jnp.broadcast_to(jnp.sum(g * values, axis=0, keepdims=True), (8, WIDE))
    skip_grad = wide_gathered(skip_row)[0:1]
    last = jnp.zeros((1, 128), f32)
    for h in range(NH):
        part = slice(h * HEAD_DIM, (h + 1) * HEAD_DIM)
        own = states[0, pl.ds(k * COLS + h * HEAD_DIM, HEAD_DIM), :]
        product = l[part] * (total_exp[:, h:h + 1] * e[part] + own)
        product = jnp.sum(jnp.sum(product, axis=0, keepdims=True), axis=1, keepdims=True)
        last += jnp.where(lane == h, product, 0.0)
    decay_grad = exact_sum(low_triangle().astype(bf16), cum_grad, ((0,), (0,))) + last
    step_grad += decay_grad * rate
    raw_step_grad = jnp.where(lanes((SPAN, 128)) < NH, step_grad * sigmoid(raw_step), 0.0)
    rounded[:, :256] = raw_value_grad[:, :256].astype(bf16)
    rounded[:, 256:384] = (raw_value_grad[:, 256:384] + pltpu.roll(raw_step_grad, 96, 1)).astype(bf16)
    map_part[0:STATE, :] = in_grad.T.astype(bf16)
    map_part[STATE:, :] = out_grad.T.astype(bf16)
    heads_out[0:1, :] += jnp.sum(raw_step_grad, axis=0, keepdims=True)
    heads_out[1:2, :] += jnp.sum(decay_grad * log_decay, axis=0, keepdims=True)
    heads_out[2:3, :] += skip_grad


def weight_kernel(rounded, ordered, total):
    part = dot(ordered[...], rounded[...], ((1,), (0,)))
    k = pl.program_id(0)

    @pl.when(k == 0)
    def _():
        total[...] = part

    @pl.when(k > 0)
    def _():
        total[...] += part


def map_kernel(rounded_in, map_parts, projected, ordered, heads, partial, rounded, weight_out, total):
    k = pl.program_id(0)
    raw = projected[...]
    gate = sigmoid(raw)
    maps = jnp.sum(map_parts[...].astype(f32), axis=0)
    zero = jnp.zeros((32, SPAN), f32)
    maps = jnp.concatenate([zero, zero, maps, zero], axis=0).T
    maps = maps * (gate * (1.0 + raw * (1.0 - gate)))
    lane = lanes((SPAN, 128))
    own = (lane >= COLS - 256) & (lane < COLS - 256 + MAPS)
    maps = jnp.where(own, maps, 0.0).astype(bf16)
    rounded[:, :256] = rounded_in[:, :256]
    rounded[:, 256:384] = jnp.where(own, maps, rounded_in[:, 256:384])
    part = dot(ordered[...], maps, ((1,), (0,)))

    @pl.when(k == 0)
    def _():
        total[...] = partial[:, 256:384] + part

    @pl.when(k > 0)
    def _():
        total[...] += part

    @pl.when(k == SEGS - 1)
    def _():
        sums = jnp.zeros((1, 128), f32)
        for i in range(3):
            sums += pltpu.roll(
                jnp.where(lanes((1, 128)) < NH, heads[i:i + 1], 0.0), HEAD_LANE + i * NH - 256, 1
            )
        hi, lo = halves(sums)
        row = lax.broadcasted_iota(jnp.int32, (8, 128), 0)
        extra = jnp.where(row == 0, hi.astype(f32), jnp.where(row == 1, lo.astype(f32), 0.0))
        row = lax.broadcasted_iota(jnp.int32, (128, 128), 0)
        owner, slot = row // 32, row % 32
        source = jnp.where(
            slot < 30, (slot // 10) * 40 + owner * 10 + slot % 10, slot + 90
        )
        pick = (source == lanes((128, 128))).astype(bf16)

        def four_owners(i, carry):
            at = pl.ds(pl.multiple_of(i * 40, 8), 40)
            tiles = [partial[at, :128], partial[at, 128:256], total[at, :]]
            block = jnp.concatenate(tiles + [extra], axis=0).astype(bf16)
            out = dot(pick, block, ((1,), (0,))).astype(bf16)
            weight_out[pl.ds(pl.multiple_of(i * 128, 128), 128), :] = out
            return carry

        lax.fori_loop(0, 32, four_owners, 0, unroll=8)


def token_kernel(where, rounded, w, kept, given):
    out = dot(rounded[...], w[...], ((1,), (1,)))
    for core in (0, 1):
        @pl.when(where[0] == core)
        def _():
            kept[0] = out[core * 128:core * 128 + 128]
            given[0] = out[(1 - core) * 128:(1 - core) * 128 + 128].astype(bf16)


def collect_kernel(parts, out):
    for group in range(8):
        total = jnp.zeros((32, 128), f32)
        for z in range(2):
            for i in range(8):
                total += parts[((group // 2 * 2 + z) * 2 + group % 2) * 8 + i].astype(f32)
        out[group] = total


def call(kernel, outs, ins, scratch=(), where=None):
    def spec(block, index):
        return pl.BlockSpec(block, index if index.__code__.co_argcount == 2 else lambda k, *at: index(k))

    return pl.pallas_call(
        kernel,
        grid_spec=pltpu.PrefetchScalarGridSpec(
            num_scalar_prefetch=0 if where is None else 1,
            grid=(SEGS,),
            in_specs=[spec(block, index) for _, block, index in ins],
            out_specs=[spec(block, index) for _, block, index in outs],
            scratch_shapes=list(scratch),
        ),
        out_shape=[shape for shape, _, _ in outs],
        compiler_params=pltpu.CompilerParams(
            dimension_semantics=("arbitrary",), vmem_limit_bytes=20 * 1024 * 1024
        ),
    )(*([] if where is None else [where]), *[v for v, _, _ in ins])


def whole(v):
    zeros = (0,) * len(v.shape)
    return (v, v.shape, lambda k: zeros)


def rows_of(v):
    return (v, (v.shape[0] // SEGS,) + v.shape[1:], lambda k: (k, 0))


def array(*dims, dtype=f32):
    return jax.ShapeDtypeStruct(dims, dtype)


def body(hidden, output_grad, input_weight, step_bias, decay_log, skip_gain):
    core = lax.axis_index("c")
    row = lax.axis_index("y")
    part_z = lax.axis_index("zl")
    group = lax.axis_index(GROUP)

    wide = WIDE + 2 * STATE
    w = lax.all_to_all(selected(input_weight, jnp.stack([group, core])), ZERO, 0, 0, tiled=True)
    w = w.reshape(D, WIDE + STATE)
    w_other = swap(w[:, WIDE:])

    own = hidden[0]
    parts = [own] + [along_y(own, d) for d in range(1, 4)]
    others = jnp.stack([swap(v) for v in parts])
    owns = jnp.stack(parts)
    kept, given = parted(output_grad[0], jnp.stack([core, row]))
    given = swap(given)
    cots = []
    for d in range(SEGS):
        part = by_core(kept[d], given[d], core, 0)
        cots.append(along_y(part, d) if d else part)
    cots = jnp.stack(cots)
    bias = lax.dynamic_slice(step_bias, (group * NH,), (NH,))
    rate = -jnp.exp(lax.dynamic_slice(decay_log, (group * NH,), (NH,)))
    skip = jnp.repeat(lax.dynamic_slice(skip_gain, (group * NH,), (NH,)), HEAD_DIM)
    params = jnp.concatenate(
        [
            jnp.pad(bias, (0, 128 - NH))[None],
            jnp.pad(rate, (0, 128 - NH))[None],
            jnp.pad(skip, (0, 64)).reshape(3, 128),
            jnp.zeros((3, 128), f32),
        ]
    )

    params = pl.pallas_call(fixed_kernel, name="fixed", out_shape=array(8, 128))(params)

    positions = SEGS * SPAN
    count = SEGS * COLS

    def both(dtype):
        return (array(2, count, STATE, dtype=dtype), (2, COLS, STATE), lambda k: (0, k, 0))

    place = jnp.stack([core, row, part_z])
    placed_cot = (cots, (1, SPAN, WIDE), lambda k, at: ((at[1] + SEGS - k) % SEGS, 0, 0))
    projected, cum, states, sends, totals, tokens = call(
        forward_kernel,
        [
            rows_of(array(positions, wide)),
            rows_of(array(positions, 128)),
            both(f32),
            both(bf16),
            whole(array(8, 128)),
            rows_of(array(positions, D, dtype=bf16)),
        ],
        [
            (owns, (1, 128, D), lambda k, at: ((at[1] + SEGS - k) % SEGS, 0, 0)),
            (others, (1, 128, D), lambda k, at: ((at[1] + SEGS - k) % SEGS, 0, 0)),
            whole(w),
            whole(w_other),
            placed_cot,
            whole(params),
        ],
        where=place,
    )
    got = swap(sends, "zl")
    got_totals = swap(totals, "zl")

    ordered = tokens.T

    out_inside, grad_inside, map_inside = call(
        inside_kernel,
        [
            rows_of(array(positions, WIDE)),
            rows_of(array(positions, WIDE)),
            rows_of(array(positions, SPAN)),
        ],
        [rows_of(projected), rows_of(cum), placed_cot, whole(params)],
        where=place,
    )
    rounded, map_part, heads = call(
        backward_kernel,
        [
            rows_of(array(positions, WIDE, dtype=bf16)),
            (array(2 * STATE, positions, dtype=bf16), (2 * STATE, SPAN), lambda k: (0, k)),
            whole(array(8, 128)),
        ],
        [
            rows_of(projected),
            rows_of(cum),
            placed_cot,
            whole(params),
            rows_of(out_inside),
            rows_of(grad_inside),
            rows_of(map_inside),
            whole(states),
            whole(got),
            whole(totals),
            whole(got_totals),
        ],
        [pltpu.VMEM((SEGS * WIDE, STATE), f32)] * 2,
        where=place,
    )
    map_part = lax.all_to_all(map_part.reshape(8, MAPS, positions), GROUP, 0, 0, tiled=True)
    (weight_part,) = call(
        weight_kernel,
        [whole(array(D, WIDE))],
        [rows_of(rounded), (ordered, (D, SPAN), lambda k: (0, k))],
    )

    rounded, weight_part = call(
        map_kernel,
        [rows_of(array(positions, WIDE, dtype=bf16)), whole(array(128 * 32, 128, dtype=bf16))],
        [
            rows_of(rounded),
            (map_part, (8, MAPS, SPAN), lambda k: (0, 0, k)),
            (projected, (SPAN, 128), lambda k: (k, 2)),
            (ordered, (D, SPAN), lambda k: (0, k)),
            whole(heads),
            whole(weight_part),
        ],
        [pltpu.VMEM((D, 128), f32)],
    )
    part = lax.all_to_all(
        weight_part.reshape(128, 32, 128), ("y", "zl", "c", "x", "zh"), 0, 0, tiled=True
    )
    kept, given = call(
        token_kernel,
        [
            (array(SEGS, 128, D), (1, 128, D), lambda k: (k, 0, 0)),
            (array(SEGS, 128, D, dtype=bf16), (1, 128, D), lambda k: (k, 0, 0)),
        ],
        [rows_of(rounded), (w, (D, WIDE), lambda k: (0, 0))],
        where=core.reshape(1),
    )
    other = swap(given)

    def term(d):
        at = (row + d) % 4
        a = lax.dynamic_index_in_dim(kept, at, 0, keepdims=False)
        return a + lax.dynamic_index_in_dim(other, at, 0, keepdims=False).astype(f32)

    token_grad = term(0)
    terms = [term(d).astype(bf16) for d in range(1, 4)]
    returned = [along_y(v, d) for d, v in zip(range(1, 4), terms)]
    part, *terms = lax.optimization_barrier((part, *terms))
    part = pl.pallas_call(
        collect_kernel, name="collect", out_shape=array(8, 32, 128)
    )(part)
    for v in returned:
        token_grad = token_grad + v.astype(f32)
    token_grad = token_grad.astype(bf16)
    at = HEAD_LANE - 256
    heads = (part[:, 30] + part[:, 31])[:, at:at + 3 * NH].reshape(8, 3, NH)
    head_grads = heads.transpose(1, 0, 2).reshape(3, 8 * NH)
    part = part[:, :30].reshape(8, 3, 10, 128).transpose(2, 0, 1, 3).reshape(10, 8, WIDE)
    weight_grad = jnp.concatenate(
        [
            part[:, :, :COLS].reshape(10, 8 * COLS),
            part[:, :, COLS:COLS + MAPS].reshape(10, 8 * MAPS),
            part[:, :, COLS + MAPS:USED].reshape(10, 8 * NH),
        ],
        axis=1,
    )
    return token_grad[None], weight_grad, head_grads


def solution(mesh):
    torus = Mesh(mesh.devices.reshape(4, 2, 2, 4, 2), ("y", "zl", "c", "x", "zh"))
    seq = ("y", "zl", "c")
    in_specs = (P(ZERO, seq, None), P(ZERO, seq, None), P(ZERO, None), P(), P(), P())
    out_specs = (P(ZERO, seq, None), P(seq + ZERO, None), P())
    return jax.shard_map(body, mesh=torus, in_specs=in_specs, out_specs=out_specs, check_vma=False)
```
